32 devices in a mesh: batch: 2 (over core), token: 8 (over z, x), hidden: 2 (over y).
Axes of the slice: x: 2, y: 2, z: 4, core: 2. Of those that a mesh axis runs over, the one named last changes fastest.
Arguments:
- hist_len: int32 [128], replicated, may hold values from 32 to 512, as said below
- queries: bfloat16 [32, 1536], P(None, 'token'), may hold values from -4 to 4
- history_keys: bfloat16 [384, 1536, 128], P(('batch', 'hidden'), 'token'), may hold values from -192 to 192
- cached_history_values: bfloat16 [384, 1536, 128], P(('batch', 'hidden'), 'token'), may hold values from -6 to 6
- gain_mix: float32 [1536], replicated, may hold values from 0.25 to 1.75
- w_up: bfloat16 [32, 1536, 3072], P('token', None, 'hidden'), may hold values from -0.15625 to 0.15625
- w_down: bfloat16 [32, 3072, 1536], P('token', 'hidden'), may hold values from -0.109375 to 0.109375
- gain_out: float32 [1536], replicated, may hold values from 0.25 to 1.75
Outputs:
- mixer_out: bfloat16 [128, 32, 1536], P(('batch', 'hidden'), 'token')
The draws below stay inside these ranges and needn't reach their ends.
Inputs may be any that keep to these rules, and one draw needn't show every extreme that they name: `hist_len`: along batch+hidden, the requests of each index need between 32 and 96 slots, indices 2i and 2i + 1 need 4 * 32 slots together, and some index needs exactly 96; within an index, requests 2j and 2j + 1 need from 2 to 6 slots together.
All inputs are finite; a program needn't handle non-finite values.
Results may differ from the reference program's by a relative error of at most 0.015.
Values may be sent and summed in bfloat16 or wider, within the bound.
No kernel may reach another device: no remote copies, remote signals or barrier semaphores. Data moves between devices by JAX's collectives and lax.ppermute only.
A program may use at most 128 MiB of HBM per device.

```python
import jax
import jax.numpy as jnp
from jax import lax

TOKEN_COUNT = 32
MODEL_WIDTH = 1536
FF = 3072
BLOCK_POSITIONS = 128
REQ_DEV = 32
SLOTS = 96
REQUESTS = 128
SLOT_TOTAL = 384
N_BATCH = 2
N_HIDDEN = 2


def make_queries(seed_key):
    return jnp.clip(jax.random.normal(seed_key, (TOKEN_COUNT, MODEL_WIDTH), jnp.float32), -4.0, 4.0)


def draw_queries(key, part):
    return make_queries(jax.random.fold_in(key, 17)).astype(jnp.bfloat16)


def draw_history_keys(key, part):
    drawn_version = jnp.clip(jax.random.normal(jax.random.fold_in(key, 23), (SLOT_TOTAL, MODEL_WIDTH, BLOCK_POSITIONS), jnp.float32), -6.0, 6.0)
    return drawn_version.astype(jnp.bfloat16)


def draw_hist_len(key, part):
    group_size = N_BATCH * N_HIDDEN
    pair_count = group_size // 2
    heavy = jax.random.randint(jax.random.fold_in(key, 41), (pair_count,), 0, 5)
    forced = jax.random.randint(jax.random.fold_in(key, 43), (), 0, pair_count)
    heavy = jnp.where(jnp.arange(pair_count) == forced, 4, heavy)
    level = jnp.stack([heavy, 4 - heavy], axis=1).reshape(group_size)
    lowest = jnp.maximum(level - 3, 0)
    highest = jnp.minimum(level, 3)
    leading_part = jax.random.randint(jax.random.fold_in(key, 47), (group_size, REQ_DEV // 2), lowest[:, None], highest[:, None] + 1)
    extra = jnp.stack([leading_part, level[:, None] - leading_part], axis=2).reshape(group_size, REQ_DEV)
    tail_rows = jax.random.randint(jax.random.fold_in(key, 53), (group_size, REQ_DEV), BLOCK_POSITIONS // 4, BLOCK_POSITIONS + 1)
    return (extra * BLOCK_POSITIONS + tail_rows).reshape(group_size * REQ_DEV).astype(jnp.int32)


def block_levels(key, shape, shards, low, high):
    level, own = 1.0, jax.random.fold_in(key, 6)
    for dim, parts in shards:
        draws = jnp.exp(jax.random.uniform(jax.random.fold_in(own, dim), (parts,), jnp.float32, low / len(shards), high / len(shards)))
        level = level * jnp.repeat(draws, shape[dim] // parts).reshape([-1 if axis == dim else 1 for axis in range(len(shape))])
    return level


def normal_values(own_key, shape, spread, limit, shards=(), held_as=jnp.bfloat16):
    entries = spread * jax.random.normal(own_key, shape, jnp.float32)
    if shards:
        entries = entries * block_levels(own_key, shape, shards, -0.22, 0.18)
    return jnp.clip(entries, -limit, limit).astype(held_as)


def setup_inputs(seed: int = 0) -> dict:
    arg_keys = jax.random.split(jax.random.key(seed), 9)
    return {
        "hist_len": draw_hist_len(jax.random.fold_in(arg_keys[8], 71), 0),
        "queries": draw_queries(jax.random.fold_in(arg_keys[8], 71), 0),
        "history_keys": draw_history_keys(jax.random.fold_in(arg_keys[8], 71), 0),
        "cached_history_values": normal_values(arg_keys[3], (SLOT_TOTAL, MODEL_WIDTH, BLOCK_POSITIONS), 1.0, 6.0, ((0, 4), (1, 8))),
        "gain_mix": jnp.clip(1.0 + 0.15 * jax.random.normal(arg_keys[4], (MODEL_WIDTH,), jnp.float32), 0.25, 1.75),
        "w_up": normal_values(arg_keys[5], (TOKEN_COUNT, MODEL_WIDTH, FF), MODEL_WIDTH ** -0.5, 0.15625, ((0, 8), (2, 2))),
        "w_down": normal_values(arg_keys[6], (TOKEN_COUNT, FF, MODEL_WIDTH), FF ** -0.5, 0.109375, ((0, 8), (1, 2))),
        "gain_out": jnp.clip(1.0 + 0.15 * jax.random.normal(arg_keys[7], (MODEL_WIDTH,), jnp.float32), 0.25, 1.75),
    }


EPSILON = 1e-05
NEGATIVE_FILL = -1e+30

def slot_layout(lengths, slot_count, block_rows):
    request_count = lengths.shape[0]
    blocks = ((lengths + block_rows - 1) // block_rows).astype(jnp.int32)
    block_ends = jnp.cumsum(blocks).astype(jnp.int32)
    block_starts = block_ends - blocks
    slot_index = jnp.arange(slot_count, dtype=jnp.int32)
    owners = lax.optimization_barrier(jnp.sum((block_ends[None, :] <= slot_index[:, None]).astype(jnp.int32), axis=1)).astype(jnp.int32)
    onehot = owners[:, None] == jnp.arange(request_count, dtype=jnp.int32)[None, :]
    start_of = lax.optimization_barrier(jnp.sum(jnp.where(onehot, block_starts[None, :], 0), axis=1)).astype(jnp.int32)
    length_of = lax.optimization_barrier(jnp.sum(jnp.where(onehot, lengths[None, :], 0), axis=1)).astype(jnp.int32)
    valid_rows = jnp.clip(length_of - (slot_index - start_of) * block_rows, 0, block_rows)
    return (onehot, valid_rows.astype(jnp.int32))

def block_partials(query_heads, slot_keys, slot_values, valid_rows, score_scale):
    scores = jnp.einsum('qhs,nhsp->nqhp', query_heads.astype(jnp.float32), slot_keys.astype(jnp.float32), precision=lax.Precision.HIGHEST) * score_scale
    position = jnp.arange(slot_keys.shape[-1], dtype=jnp.int32)
    in_range = position[None, None, None, :] < valid_rows[:, None, None, None]
    scores = jnp.where(in_range, scores, NEGATIVE_FILL)
    maxima = lax.optimization_barrier(jnp.max(scores, axis=-1))
    softmax_terms = jnp.where(in_range, jnp.exp(scores - maxima[..., None]), 0.0)
    totals = lax.optimization_barrier(jnp.sum(softmax_terms, axis=-1))
    rounded_terms = softmax_terms.astype(jnp.bfloat16).astype(jnp.float32)
    weighted = jnp.einsum('nqhp,nhsp->nqhs', rounded_terms, slot_values.astype(jnp.float32), precision=lax.Precision.HIGHEST)
    return (maxima, totals, weighted)

def combine_blocks(maxima, totals, weighted, onehot):
    owned = onehot.astype(jnp.float32)
    is_live = lax.optimization_barrier(jnp.sum(owned, axis=1)) > 0.5
    masked_max = jnp.where(onehot[:, :, None, None], maxima[:, None, :, :], NEGATIVE_FILL)
    request_max = lax.optimization_barrier(jnp.max(masked_max, axis=0))
    owner_max = jnp.einsum('nr,rqh->nqh', owned, request_max, precision=lax.Precision.HIGHEST)
    factor = jnp.exp(jnp.where(is_live[:, None, None], maxima - owner_max, NEGATIVE_FILL))
    denominator = jnp.einsum('nr,nqh->rqh', owned, factor * totals, precision=lax.Precision.HIGHEST)
    numerator = jnp.einsum('nr,nqhs->rqhs', owned, factor[..., None] * weighted, precision=lax.Precision.HIGHEST)
    return (numerator / denominator[..., None]).astype(jnp.bfloat16)

def layer_norm(summand):
    average = lax.optimization_barrier(jnp.mean(summand, axis=-1, keepdims=True))
    centred = summand - average
    variance = lax.optimization_barrier(jnp.mean(centred * centred, axis=-1, keepdims=True))
    return centred * lax.rsqrt(variance + EPSILON)

def reference(hist_len, queries, history_keys, cached_history_values, gain_mix, w_up, w_down, gain_out):
    head_size = MODEL_WIDTH // TOKEN_COUNT
    group_count = hist_len.shape[0] // REQ_DEV
    query_heads = queries.reshape(TOKEN_COUNT, TOKEN_COUNT, head_size)
    score_scale = head_size ** (-0.5)

    def one_group(group_id):
        lengths = lax.dynamic_slice_in_dim(hist_len, group_id * REQ_DEV, REQ_DEV)
        slot_keys = lax.dynamic_slice_in_dim(history_keys, group_id * SLOTS, SLOTS).reshape(SLOTS, TOKEN_COUNT, head_size, BLOCK_POSITIONS)
        slot_values = lax.dynamic_slice_in_dim(cached_history_values, group_id * SLOTS, SLOTS).reshape(SLOTS, TOKEN_COUNT, head_size, BLOCK_POSITIONS)
        onehot, valid_rows = slot_layout(lengths, SLOTS, BLOCK_POSITIONS)
        maxima, totals, weighted = block_partials(query_heads, slot_keys, slot_values, valid_rows, score_scale)
        return combine_blocks(maxima, totals, weighted, onehot)
    attended = lax.map(one_group, jnp.arange(group_count, dtype=jnp.int32))
    attended = attended.reshape(REQUESTS, TOKEN_COUNT, TOKEN_COUNT, head_size)
    mixed_rows = jnp.transpose(attended, (0, 2, 1, 3)).reshape(REQUESTS, TOKEN_COUNT, MODEL_WIDTH)
    unmixed = attended.reshape(REQUESTS, TOKEN_COUNT, MODEL_WIDTH)
    joined = mixed_rows.astype(jnp.float32) + unmixed.astype(jnp.float32)
    normed = (layer_norm(joined) * gain_mix).astype(jnp.bfloat16)

    def token_ffn(operands):
        token_rows, up_weight, down_weight = operands
        lifted = jnp.dot(token_rows, up_weight, preferred_element_type=jnp.float32)
        activated = jax.nn.gelu(lifted, approximate=False).astype(jnp.bfloat16)
        return jnp.dot(activated, down_weight, preferred_element_type=jnp.float32)
    ffn_out = lax.map(token_ffn, (jnp.transpose(normed, (1, 0, 2)), w_up, w_down))
    ffn_out = jnp.transpose(ffn_out, (1, 0, 2))
    return (layer_norm(ffn_out + normed.astype(jnp.float32)) * gain_out).astype(jnp.bfloat16)
```

```python
import math

import jax
import jax.numpy as jnp
from jax import lax
from jax.experimental import pallas as pl
from jax.experimental.pallas import tpu as pltpu
from jax.sharding import PartitionSpec as P

EPSILON = 1e-05
NEGATIVE_FILL = -1e30
LONGEST = 512
BLOCK_REQUESTS = 4
MIB = 1 << 20


def peer_of(index, step, count):
    if count & (count - 1) == 0:
        return index ^ step
    return (index + step) % count


def source_of(index, step, count):
    if count & (count - 1) == 0:
        return index ^ step
    return (index + count - step) % count


def exchange(value, axis, step, count):
    return lax.ppermute(value, axis, [(a, peer_of(a, step, count)) for a in range(count)])


def attention_kernel(sizes, len_ref, query_ref, key_hbm, value_hbm, *rest):
    tokens, heads, requests, head_size, positions, slots = sizes
    outs = rest[:tokens]
    key_buf, value_buf, query_f32, query_diag, first_ref, send, sems = rest[tokens:]
    width = heads * head_size
    lane_tiles = send.shape[0]
    blocks = requests // BLOCK_REQUESTS
    chunk = slots // blocks
    depth = -(-LONGEST // positions)

    def copies(block):
        where = pl.ds(block * chunk, chunk)
        return (
            pltpu.make_async_copy(key_hbm.at[where], key_buf.at[where], sems.at[0, block]),
            pltpu.make_async_copy(value_hbm.at[where], value_buf.at[where], sems.at[1, block]),
        )

    for block in range(blocks):
        for copy in copies(block):
            copy.start()

    group = lax.axis_index(("batch", "hidden"))
    base = group * requests

    def place(r, first):
        first_ref[r] = first
        return first + (len_ref[base + r] + (positions - 1)) // positions

    lax.fori_loop(0, requests, place, jnp.int32(0))

    query_f32[...] = query_ref[...].astype(jnp.float32)
    column_head = lax.broadcasted_iota(jnp.int32, (tokens, width), 1) // head_size
    for i in range(heads):
        rows = jnp.concatenate(
            [query_f32[d * heads + i : d * heads + i + 1, :] for d in range(tokens)], axis=0
        )
        for h in range(heads):
            start = (i * heads + h) * tokens
            query_diag[start : start + tokens, :] = jnp.where(column_head == h, rows, 0.0)
    queries = query_diag[...].astype(jnp.bfloat16)
    factor = math.log2(math.e) * head_size ** (-0.5)
    lane = lax.broadcasted_iota(jnp.int32, (1, depth * positions), 1)

    def block_body(block, carry):
        for copy in copies(block):
            copy.wait()
        last = (block + 1) * chunk - 1
        for offset in range(BLOCK_REQUESTS):
            r = block * BLOCK_REQUESTS + offset
            first = first_ref[r]
            length = len_ref[base + r]
            index = [jnp.minimum(first + b, last) for b in range(depth)]
            keys = jnp.concatenate([key_buf[n] for n in index], axis=1)
            values = jnp.concatenate([value_buf[n] for n in index], axis=1)
            scores = jnp.dot(queries, keys, preferred_element_type=jnp.float32)
            scores = jnp.where(lane < length, scores, NEGATIVE_FILL)
            top = jnp.max(scores, axis=1, keepdims=True)
            terms = jnp.exp2((scores - top) * factor)
            total = jnp.sum(terms, axis=1, keepdims=True)
            acc = lax.dot_general(
                terms.astype(jnp.bfloat16),
                values,
                (((1,), (1,)), ((), ())),
                preferred_element_type=jnp.float32,
            )
            acc = acc / total
            for i in range(heads):
                start = i * heads * tokens
                kept = acc[start : start + tokens]
                for h in range(1, heads):
                    begin = start + h * tokens
                    kept = jnp.where(column_head >= h, acc[begin : begin + tokens], kept)
                spare = lane_tiles * 128 - width
                if spare:
                    kept = jnp.concatenate([kept, jnp.zeros((tokens, spare), jnp.float32)], axis=1)
                for tile in range(lane_tiles):
                    send[tile, pl.ds(i * requests + r, tokens, stride=heads * requests), :] = kept[
                        :, tile * 128 : (tile + 1) * 128
                    ]
        return carry

    lax.fori_loop(0, blocks, block_body, jnp.int32(0))

    mine = lax.axis_index("token")
    for step in range(tokens):
        d = peer_of(mine, step, tokens)
        where = pl.ds(pl.multiple_of(d * (heads * requests), heads * requests), heads * requests)
        rows = jnp.concatenate([send[tile, where, :] for tile in range(lane_tiles)], axis=1)
        outs[step][...] = rows[:, :width].astype(jnp.bfloat16)


def attention(hist_len, queries, keys, values, tokens, requests):
    slots, width, positions = keys.shape
    heads = queries.shape[0] // tokens
    head_size = width // heads
    blocks = requests // BLOCK_REQUESTS
    lane_tiles = -(-width // 128)
    flops = 4 * requests * LONGEST * heads * heads * tokens * width
    return pl.pallas_call(
        lambda *refs: attention_kernel((tokens, heads, requests, head_size, positions, slots), *refs),
        out_shape=[jax.ShapeDtypeStruct((heads * requests, width), jnp.bfloat16)] * tokens,
        in_specs=[
            pl.BlockSpec(memory_space=pltpu.SMEM),
            pl.BlockSpec(memory_space=pltpu.VMEM),
            pl.BlockSpec(memory_space=pl.ANY),
            pl.BlockSpec(memory_space=pl.ANY),
        ],
        out_specs=[pl.BlockSpec(memory_space=pltpu.VMEM)] * tokens,
        scratch_shapes=[
            pltpu.VMEM(keys.shape, keys.dtype),
            pltpu.VMEM(values.shape, values.dtype),
            pltpu.VMEM(queries.shape, jnp.float32),
            pltpu.VMEM((heads * heads * tokens, width), jnp.float32),
            pltpu.SMEM((requests,), jnp.int32),
            pltpu.VMEM((lane_tiles, tokens * heads * requests, 128), jnp.float32),
            pltpu.SemaphoreType.DMA((2, blocks)),
        ],
        compiler_params=pltpu.CompilerParams(vmem_limit_bytes=24 * MIB),
        cost_estimate=pl.CostEstimate(
            flops=flops, transcendentals=flops // 400, bytes_accessed=2 * keys.size * 2
        ),
        name="attention",
    )(hist_len, queries, keys, values)


def norm_rows(rows):
    average = jnp.mean(rows, axis=-1, keepdims=True)
    centred = rows - average
    variance = jnp.mean(centred * centred, axis=-1, keepdims=True)
    return centred * lax.rsqrt(variance + EPSILON)


def mix_kernel(sizes, *refs):
    tokens, heads, requests, head_size, j = sizes
    sent = refs[:tokens]
    received = refs[tokens : 2 * tokens]
    gain_ref, out_ref, joined = refs[2 * tokens :]
    mine = lax.axis_index("token")
    for step in range(tokens):
        s = source_of(mine, step, tokens)
        own = sent[peer_step(step, tokens)]
        mixed = jnp.concatenate(
            [
                own[h * requests : (h + 1) * requests, j * head_size : (j + 1) * head_size]
                for h in range(heads)
            ],
            axis=1,
        )
        unmixed = received[step][j * requests : (j + 1) * requests, :]
        joined[s] = mixed.astype(jnp.float32) + unmixed.astype(jnp.float32)
    rows = jnp.concatenate([joined[s] for s in range(tokens)], axis=1)
    out_ref[...] = (norm_rows(rows) * gain_ref[...]).astype(jnp.bfloat16)


def peer_step(step, count):
    if count & (count - 1) == 0:
        return step
    return (count - step) % count


def mix(sent, received, gain, j, tokens, requests):
    heads = sent[0].shape[0] // requests
    width = sent[0].shape[1]
    model = gain.shape[1]
    return pl.pallas_call(
        lambda *refs: mix_kernel((tokens, heads, requests, width // heads, j), *refs),
        out_shape=jax.ShapeDtypeStruct((requests, model), jnp.bfloat16),
        scratch_shapes=[pltpu.VMEM((tokens, requests, width), jnp.float32)],
        compiler_params=pltpu.CompilerParams(vmem_limit_bytes=8 * MIB),
        cost_estimate=pl.CostEstimate(
            flops=10 * requests * model, transcendentals=0, bytes_accessed=6 * requests * model
        ),
        name="mix",
    )(*sent, *received, gain)


def ffn_kernel(sizes, *refs):
    j, peers, chunks = sizes
    rows = refs[:peers]
    up_hbm, down_hbm = refs[peers : peers + 2]
    outs = refs[peers + 2 : 2 * peers + 2]
    up_buf, down_buf, sems = refs[2 * peers + 2 :]
    hidden = up_buf.shape[1]
    size = hidden // chunks

    def copies(c):
        where = pl.ds(c * size, size)
        return (
            pltpu.make_async_copy(up_hbm.at[j, :, where], up_buf.at[:, where], sems.at[0, c]),
            pltpu.make_async_copy(down_hbm.at[j, where, :], down_buf.at[where, :], sems.at[1, c]),
        )

    for c in range(chunks):
        for copy in copies(c):
            copy.start()
    x = jnp.concatenate([ref[...] for ref in rows], axis=0)
    total = None
    for c in range(chunks):
        up, down = copies(c)
        where = slice(c * size, (c + 1) * size)
        up.wait()
        lifted = jnp.dot(x, up_buf[:, where], preferred_element_type=jnp.float32)
        activated = (0.5 * lifted * (1.0 + lax.erf(lifted * math.sqrt(0.5)))).astype(jnp.bfloat16)
        down.wait()
        part = jnp.dot(activated, down_buf[where, :], preferred_element_type=jnp.float32)
        total = part if total is None else total + part
    count = rows[0].shape[0]
    for k in range(peers):
        outs[k][...] = total[k * count : (k + 1) * count].astype(outs[k].dtype)


def ffn(rows, w_up, w_down, j):
    _, model, hidden = w_up.shape
    chunks = 4 if hidden % 512 == 0 else 1
    peers = len(rows)
    count = rows[0].shape[0]
    return pl.pallas_call(
        lambda *refs: ffn_kernel((j, peers, chunks), *refs),
        out_shape=[
            jax.ShapeDtypeStruct((count, model), jnp.float32 if k == 0 else jnp.bfloat16)
            for k in range(peers)
        ],
        in_specs=[pl.BlockSpec(memory_space=pltpu.VMEM)] * peers
        + [pl.BlockSpec(memory_space=pl.ANY)] * 2,
        out_specs=[pl.BlockSpec(memory_space=pltpu.VMEM)] * peers,
        scratch_shapes=[
            pltpu.VMEM((model, hidden), w_up.dtype),
            pltpu.VMEM((hidden, model), w_down.dtype),
            pltpu.SemaphoreType.DMA((2, chunks)),
        ],
        compiler_params=pltpu.CompilerParams(vmem_limit_bytes=24 * MIB),
        cost_estimate=pl.CostEstimate(
            flops=4 * peers * count * model * hidden,
            transcendentals=peers * count * hidden,
            bytes_accessed=4 * model * hidden,
        ),
        name="ffn",
    )(*rows, w_up, w_down)


def finish_kernel(sizes, *refs):
    heads, parts = sizes
    gain_ref, out_ref = refs[heads * parts :]
    for j in range(heads):
        summed = refs[j * parts][...]
        for ref in refs[j * parts + 1 : (j + 1) * parts]:
            summed = summed + ref[...].astype(jnp.float32)
        out_ref[:, j, :] = (norm_rows(summed) * gain_ref[...]).astype(jnp.bfloat16)


def finish(terms, gain):
    heads, parts = len(terms), len(terms[0])
    count, model = terms[0][0].shape
    return pl.pallas_call(
        lambda *refs: finish_kernel((heads, parts), *refs),
        out_shape=jax.ShapeDtypeStruct((count, heads, model), jnp.bfloat16),
        compiler_params=pltpu.CompilerParams(vmem_limit_bytes=16 * MIB),
        cost_estimate=pl.CostEstimate(
            flops=10 * heads * count * model, transcendentals=0, bytes_accessed=8 * heads * count * model
        ),
        name="finish",
    )(*[part for token in terms for part in token], gain)


def local(hist_len, queries, history_keys, cached_history_values, gain_mix, w_up, w_down, gain_out):
    tokens = lax.axis_size("token")
    sides = lax.axis_size("hidden")
    groups = lax.axis_size("batch") * sides
    requests = hist_len.shape[0] // groups
    heads = queries.shape[0] // tokens
    sent = attention(hist_len, queries, history_keys, cached_history_values, tokens, requests)
    received = [sent[0]] + [exchange(sent[k], "token", k, tokens) for k in range(1, tokens)]
    gain_mix = gain_mix.reshape(1, -1)
    gain_out = gain_out.reshape(1, -1)
    normed = [mix(sent, received, gain_mix, j, tokens, requests) for j in range(heads)]
    terms = []
    for j in range(heads):
        rows = [normed[j]] + [exchange(normed[j], "hidden", k, sides) for k in range(1, sides)]
        parts = ffn(rows, w_up, w_down, j)
        back = [
            exchange(parts[k], "hidden", peer_step(k, sides), sides) for k in range(1, sides)
        ]
        terms.append([parts[0]] + back + [normed[j]])
    return finish(terms, gain_out)


def solution(mesh):
    return jax.shard_map(
        local,
        mesh=mesh,
        in_specs=(
            P(),
            P(None, "token"),
            P(("batch", "hidden"), "token", None),
            P(("batch", "hidden"), "token", None),
            P(),
            P("token", None, "hidden"),
            P("token", "hidden", None),
            P(),
        ),
        out_specs=P(("batch", "hidden"), "token", None),
        check_vma=False,
    )
```

```python
import math

import jax
import jax.numpy as jnp
from jax import lax
from jax.experimental import pallas as pl
from jax.experimental.pallas import tpu as pltpu
from jax.sharding import PartitionSpec as P

EPSILON = 1e-05
NEGATIVE_FILL = -1e30
LONGEST = 512
BLOCK_REQUESTS = 4
MIB = 1 << 20


def peer_of(index, step, count):
    if count & (count - 1) == 0:
        return index ^ step
    return (index + step) % count


def source_of(index, step, count):
    if count & (count - 1) == 0:
        return index ^ step
    return (index + count - step) % count


def exchange(value, axis, step, count):
    return lax.ppermute(value, axis, [(a, peer_of(a, step, count)) for a in range(count)])


def attention_kernel(sizes, len_hbm, query_hbm, key_hbm, value_hbm, *rest):
    tokens, heads, requests, head_size, positions, slots = sizes
    outs = rest[:tokens]
    len_ref, query_ref, key_buf, value_buf, query_f32, query_diag, first_ref, send, sems, small = rest[
        tokens:
    ]
    width = heads * head_size
    lane_tiles = send.shape[0]
    blocks = requests // BLOCK_REQUESTS
    chunk = slots // blocks
    depth = -(-LONGEST // positions)

    def copies(block):
        where = pl.ds(block * chunk, chunk)
        return (
            pltpu.make_async_copy(key_hbm.at[where], key_buf.at[where], sems.at[0, block]),
            pltpu.make_async_copy(value_hbm.at[where], value_buf.at[where], sems.at[1, block]),
        )

    len_copy = pltpu.make_async_copy(len_hbm, len_ref, small.at[0])
    query_copy = pltpu.make_async_copy(query_hbm, query_ref, small.at[1])
    len_copy.start()
    query_copy.start()
    for block in range(blocks):
        for copy in copies(block):
            copy.start()
    len_copy.wait()

    group = lax.axis_index(("batch", "hidden"))
    base = group * requests

    def place(r, first):
        first_ref[r] = first
        return first + (len_ref[base + r] + (positions - 1)) // positions

    lax.fori_loop(0, requests, place, jnp.int32(0))

    query_copy.wait()
    query_f32[...] = query_ref[...].astype(jnp.float32)
    column_head = lax.broadcasted_iota(jnp.int32, (tokens, width), 1) // head_size
    for i in range(heads):
        rows = jnp.concatenate(
            [query_f32[d * heads + i : d * heads + i + 1, :] for d in range(tokens)], axis=0
        )
        for h in range(heads):
            start = (i * heads + h) * tokens
            query_diag[start : start + tokens, :] = jnp.where(column_head == h, rows, 0.0)
    queries = query_diag[...].astype(jnp.bfloat16)
    factor = math.log2(math.e) * head_size ** (-0.5)
    lane = lax.broadcasted_iota(jnp.int32, (1, depth * positions), 1)

    def block_body(block, carry):
        for copy in copies(block):
            copy.wait()
        last = (block + 1) * chunk - 1
        for offset in range(BLOCK_REQUESTS):
            r = block * BLOCK_REQUESTS + offset
            first = first_ref[r]
            length = len_ref[base + r]
            index = [jnp.minimum(first + b, last) for b in range(depth)]
            keys = jnp.concatenate([key_buf[n] for n in index], axis=1)
            values = jnp.concatenate([value_buf[n] for n in index], axis=1)
            scores = jnp.dot(queries, keys, preferred_element_type=jnp.float32)
            scores = jnp.where(lane < length, scores, NEGATIVE_FILL)
            top = jnp.max(scores, axis=1, keepdims=True)
            terms = jnp.exp2((scores - top) * factor)
            total = jnp.sum(terms, axis=1, keepdims=True)
            acc = lax.dot_general(
                terms.astype(jnp.bfloat16),
                values,
                (((1,), (1,)), ((), ())),
                preferred_element_type=jnp.float32,
            )
            acc = acc / total
            for i in range(heads):
                start = i * heads * tokens
                kept = acc[start : start + tokens]
                for h in range(1, heads):
                    begin = start + h * tokens
                    kept = jnp.where(column_head >= h, acc[begin : begin + tokens], kept)
                spare = lane_tiles * 128 - width
                if spare:
                    kept = jnp.concatenate([kept, jnp.zeros((tokens, spare), jnp.float32)], axis=1)
                for tile in range(lane_tiles):
                    send[tile, pl.ds(i * requests + r, tokens, stride=heads * requests), :] = kept[
                        :, tile * 128 : (tile + 1) * 128
                    ]
        return carry

    lax.fori_loop(0, blocks, block_body, jnp.int32(0))

    mine = lax.axis_index("token")
    for step in range(tokens):
        d = peer_of(mine, step, tokens)
        where = pl.ds(pl.multiple_of(d * (heads * requests), heads * requests), heads * requests)
        rows = jnp.concatenate([send[tile, where, :] for tile in range(lane_tiles)], axis=1)
        outs[step][...] = rows[:, :width].astype(jnp.bfloat16)


def attention(hist_len, queries, keys, values, tokens, requests):
    slots, width, positions = keys.shape
    heads = queries.shape[0] // tokens
    head_size = width // heads
    blocks = requests // BLOCK_REQUESTS
    lane_tiles = -(-width // 128)
    flops = 40 * requests * LONGEST * heads * heads * tokens * width
    return pl.pallas_call(
        lambda *refs: attention_kernel((tokens, heads, requests, head_size, positions, slots), *refs),
        out_shape=[jax.ShapeDtypeStruct((heads * requests, width), jnp.bfloat16)] * tokens,
        in_specs=[pl.BlockSpec(memory_space=pltpu.MemorySpace.HBM)] * 4,
        out_specs=[pl.BlockSpec(memory_space=pltpu.VMEM)] * tokens,
        scratch_shapes=[
            pltpu.SMEM(hist_len.shape, jnp.int32),
            pltpu.VMEM(queries.shape, queries.dtype),
            pltpu.VMEM(keys.shape, keys.dtype),
            pltpu.VMEM(values.shape, values.dtype),
            pltpu.VMEM(queries.shape, jnp.float32),
            pltpu.VMEM((heads * heads * tokens, width), jnp.float32),
            pltpu.SMEM((requests,), jnp.int32),
            pltpu.VMEM((lane_tiles, tokens * heads * requests, 128), jnp.float32),
            pltpu.SemaphoreType.DMA((2, blocks)),
            pltpu.SemaphoreType.DMA((2,)),
        ],
        compiler_params=pltpu.CompilerParams(vmem_limit_bytes=16 * MIB),
        cost_estimate=pl.CostEstimate(
            flops=flops, transcendentals=flops // 400, bytes_accessed=20 * keys.size * 2
        ),
        name="attention",
    )(*[pltpu.with_memory_space_constraint(x, pltpu.HBM) for x in (hist_len, queries, keys, values)])


def norm_rows(rows):
    average = jnp.mean(rows, axis=-1, keepdims=True)
    centred = rows - average
    variance = jnp.mean(centred * centred, axis=-1, keepdims=True)
    return centred * lax.rsqrt(variance + EPSILON)


def mix_kernel(sizes, *refs):
    tokens, heads, requests, head_size, j = sizes
    sent = refs[:tokens]
    received = refs[tokens : 2 * tokens]
    gain_ref, out_ref, joined = refs[2 * tokens :]
    mine = lax.axis_index("token")
    for step in range(tokens):
        s = source_of(mine, step, tokens)
        own = sent[peer_step(step, tokens)]
        mixed = jnp.concatenate(
            [
                own[h * requests : (h + 1) * requests, j * head_size : (j + 1) * head_size]
                for h in range(heads)
            ],
            axis=1,
        )
        unmixed = received[step][j * requests : (j + 1) * requests, :]
        joined[s] = mixed.astype(jnp.float32) + unmixed.astype(jnp.float32)
    rows = jnp.concatenate([joined[s] for s in range(tokens)], axis=1)
    out_ref[...] = (norm_rows(rows) * gain_ref[...]).astype(jnp.bfloat16)


def peer_step(step, count):
    if count & (count - 1) == 0:
        return step
    return (count - step) % count


def mix(sent, received, gain, j, tokens, requests):
    heads = sent[0].shape[0] // requests
    width = sent[0].shape[1]
    model = gain.shape[1]
    return pl.pallas_call(
        lambda *refs: mix_kernel((tokens, heads, requests, width // heads, j), *refs),
        out_shape=jax.ShapeDtypeStruct((requests, model), jnp.bfloat16),
        scratch_shapes=[pltpu.VMEM((tokens, requests, width), jnp.float32)],
        compiler_params=pltpu.CompilerParams(vmem_limit_bytes=8 * MIB),
        cost_estimate=pl.CostEstimate(
            flops=10 * requests * model, transcendentals=0, bytes_accessed=6 * requests * model
        ),
        name="mix",
    )(*sent, *received, gain)


def ffn_kernel(sizes, *refs):
    j, peers = sizes
    rows = refs[:peers]
    up_ref, down_ref = refs[peers : peers + 2]
    outs = refs[peers + 2 :]
    x = jnp.concatenate([ref[...] for ref in rows], axis=0)
    lifted = jnp.dot(x, up_ref[j], preferred_element_type=jnp.float32)
    activated = (0.5 * lifted * (1.0 + lax.erf(lifted * math.sqrt(0.5)))).astype(jnp.bfloat16)
    total = jnp.dot(activated, down_ref[j], preferred_element_type=jnp.float32)
    count = rows[0].shape[0]
    for k in range(peers):
        outs[k][...] = total[k * count : (k + 1) * count].astype(outs[k].dtype)


def ffn(rows, w_up, w_down, j):
    _, model, hidden = w_up.shape
    peers = len(rows)
    count = rows[0].shape[0]
    return pl.pallas_call(
        lambda *refs: ffn_kernel((j, peers), *refs),
        out_shape=[
            jax.ShapeDtypeStruct((count, model), jnp.float32 if k == 0 else jnp.bfloat16)
            for k in range(peers)
        ],
        in_specs=[pl.BlockSpec(memory_space=pltpu.VMEM)] * (peers + 2),
        out_specs=[pl.BlockSpec(memory_space=pltpu.VMEM)] * peers,
        compiler_params=pltpu.CompilerParams(vmem_limit_bytes=8 * MIB),
        cost_estimate=pl.CostEstimate(
            flops=4 * peers * count * model * hidden,
            transcendentals=peers * count * hidden,
            bytes_accessed=4 * model * hidden,
        ),
        name="ffn",
    )(*rows, w_up, w_down)


def finish_kernel(sizes, *refs):
    heads, parts = sizes
    gain_ref, out_ref = refs[heads * parts :]
    for j in range(heads):
        summed = refs[j * parts][...]
        for ref in refs[j * parts + 1 : (j + 1) * parts]:
            summed = summed + ref[...].astype(jnp.float32)
        out_ref[:, j, :] = (norm_rows(summed) * gain_ref[...]).astype(jnp.bfloat16)


def finish(terms, gain):
    heads, parts = len(terms), len(terms[0])
    count, model = terms[0][0].shape
    return pl.pallas_call(
        lambda *refs: finish_kernel((heads, parts), *refs),
        out_shape=jax.ShapeDtypeStruct((count, heads, model), jnp.bfloat16),
        compiler_params=pltpu.CompilerParams(vmem_limit_bytes=16 * MIB),
        cost_estimate=pl.CostEstimate(
            flops=10 * heads * count * model, transcendentals=0, bytes_accessed=8 * heads * count * model
        ),
        name="finish",
    )(*[part for token in terms for part in token], gain)


def local(hist_len, queries, history_keys, cached_history_values, gain_mix, w_up, w_down, gain_out):
    tokens = lax.axis_size("token")
    sides = lax.axis_size("hidden")
    groups = lax.axis_size("batch") * sides
    requests = hist_len.shape[0] // groups
    heads = queries.shape[0] // tokens
    w_up = pltpu.with_memory_space_constraint(w_up, pltpu.VMEM)
    w_down = pltpu.with_memory_space_constraint(w_down, pltpu.VMEM)
    sent = attention(hist_len, queries, history_keys, cached_history_values, tokens, requests)
    arrived = {0: sent[0]}
    for k in [1] + list(range(tokens - 1, 1, -1)):
        arrived[k] = exchange(sent[k], "token", k, tokens)
    received = [arrived[k] for k in range(tokens)]
    gain_mix = gain_mix.reshape(1, -1)
    gain_out = gain_out.reshape(1, -1)
    normed = [mix(sent, received, gain_mix, j, tokens, requests) for j in range(heads)]
    terms = []
    for j in range(heads):
        rows = [normed[j]] + [exchange(normed[j], "hidden", k, sides) for k in range(1, sides)]
        parts = ffn(rows, w_up, w_down, j)
        back = [
            exchange(parts[k], "hidden", peer_step(k, sides), sides) for k in range(1, sides)
        ]
        terms.append([parts[0]] + back + [normed[j]])
    return finish(terms, gain_out)


def solution(mesh):
    return jax.shard_map(
        local,
        mesh=mesh,
        in_specs=(
            P(),
            P(None, "token"),
            P(("batch", "hidden"), "token", None),
            P(("batch", "hidden"), "token", None),
            P(),
            P("token", None, "hidden"),
            P("token", "hidden", None),
            P(),
        ),
        out_specs=P(("batch", "hidden"), "token", None),
        check_vma=False,
    )
```

```python
import math

import jax
import jax.numpy as jnp
from jax import lax
from jax.experimental import pallas as pl
from jax.experimental.pallas import tpu as pltpu
from jax.sharding import PartitionSpec as P


EPSILON = 1e-05
NEGATIVE_FILL = -1e30
LONGEST = 512
BLOCK_REQUESTS = 4
MIB = 1 << 20


def peer_of(index, step, count):
    if count & (count - 1) == 0:
        return index ^ step
    return (index + step) % count


def source_of(index, step, count):
    if count & (count - 1) == 0:
        return index ^ step
    return (index + count - step) % count


def exchange(value, axis, step, count):
    return lax.ppermute(value, axis, [(a, peer_of(a, step, count)) for a in range(count)])


def attention_kernel(sizes, len_hbm, query_hbm, key_hbm, value_hbm, *rest):
    tokens, heads, requests, head_size, positions, slots = sizes
    send, len_ref, query_ref, key_buf, value_buf, query_f32, query_diag, first_ref, sems, small = rest
    width = heads * head_size
    lane_tiles = send.shape[0]
    blocks = requests // BLOCK_REQUESTS
    chunk = slots // blocks
    depth = -(-LONGEST // positions)

    def copies(block):
        where = pl.ds(block * chunk, chunk)
        return (
            pltpu.make_async_copy(key_hbm.at[where], key_buf.at[where], sems.at[0, block]),
            pltpu.make_async_copy(value_hbm.at[where], value_buf.at[where], sems.at[1, block]),
        )

    len_copy = pltpu.make_async_copy(len_hbm, len_ref, small.at[0])
    query_copy = pltpu.make_async_copy(query_hbm, query_ref, small.at[1])
    len_copy.start()
    query_copy.start()
    for block in range(blocks):
        for copy in copies(block):
            copy.start()
    len_copy.wait()

    group = lax.axis_index(("batch", "hidden"))
    base = group * requests

    def place(r, first):
        first_ref[r] = first
        return first + (len_ref[base + r] + (positions - 1)) // positions

    lax.fori_loop(0, requests, place, jnp.int32(0))

    query_copy.wait()
    query_f32[...] = query_ref[...].astype(jnp.float32)
    column_head = lax.broadcasted_iota(jnp.int32, (tokens, width), 1) // head_size
    for i in range(heads):
        rows = jnp.concatenate(
            [query_f32[d * heads + i : d * heads + i + 1, :] for d in range(tokens)], axis=0
        )
        for h in range(heads):
            start = (i * heads + h) * tokens
            query_diag[start : start + tokens, :] = jnp.where(column_head == h, rows, 0.0)
    queries = query_diag[...].astype(jnp.bfloat16)
    factor = math.log2(math.e) * head_size ** (-0.5)
    lane = lax.broadcasted_iota(jnp.int32, (1, depth * positions), 1)

    def block_body(block, carry):
        for copy in copies(block):
            copy.wait()
        last = (block + 1) * chunk - 1
        for offset in range(BLOCK_REQUESTS):
            r = block * BLOCK_REQUESTS + offset
            first = first_ref[r]
            length = len_ref[base + r]
            index = [jnp.minimum(first + b, last) for b in range(depth)]
            keys = jnp.concatenate([key_buf[n] for n in index], axis=1)
            values = jnp.concatenate([value_buf[n] for n in index], axis=1)
            scores = jnp.dot(queries, keys, preferred_element_type=jnp.float32)
            scores = jnp.where(lane < length, scores, NEGATIVE_FILL)
            top = jnp.max(scores, axis=1, keepdims=True)
            terms = jnp.exp2((scores - top) * factor)
            total = jnp.sum(terms, axis=1, keepdims=True)
            acc = lax.dot_general(
                terms.astype(jnp.bfloat16),
                values,
                (((1,), (1,)), ((), ())),
                preferred_element_type=jnp.float32,
            )
            acc = acc / total
            for i in range(heads):
                start = i * heads * tokens
                kept = acc[start : start + tokens]
                for h in range(1, heads):
                    begin = start + h * tokens
                    kept = jnp.where(column_head >= h, acc[begin : begin + tokens], kept)
                spare = lane_tiles * 128 - width
                if spare:
                    kept = jnp.concatenate([kept, jnp.zeros((tokens, spare), jnp.float32)], axis=1)
                for tile in range(lane_tiles):
                    send[tile, pl.ds(i * requests + r, tokens, stride=heads * requests), :] = kept[
                        :, tile * 128 : (tile + 1) * 128
                    ]
        return carry

    lax.fori_loop(0, blocks, block_body, jnp.int32(0))


def pack_kernel(sizes, send, *outs):
    tokens, rows, width = sizes
    lane_tiles = send.shape[0]
    mine = lax.axis_index("token")
    for out, step in zip(outs, message_order(tokens)):
        d = peer_of(mine, step, tokens)
        where = pl.ds(pl.multiple_of(d * rows, rows), rows)
        values = jnp.concatenate([send[tile, where, :] for tile in range(lane_tiles)], axis=1)
        out[...] = values[:, :width].astype(jnp.bfloat16)


def message_order(tokens):
    return [0] + list(range(tokens - 1, 0, -1))


def pack(send, tokens, requests, heads, width):
    rows = heads * requests
    outs = pl.pallas_call(
        lambda *refs: pack_kernel((tokens, rows, width), *refs),
        out_shape=[jax.ShapeDtypeStruct((rows, width), jnp.bfloat16)] * tokens,
        in_specs=[pl.BlockSpec(memory_space=pltpu.VMEM)],
        out_specs=[pl.BlockSpec(memory_space=pltpu.VMEM)] * tokens,
        compiler_params=pltpu.CompilerParams(vmem_limit_bytes=4 * MIB),
        cost_estimate=pl.CostEstimate(
            flops=30_000_000_000, transcendentals=0, bytes_accessed=200_000_000
        ),
        name="pack",
    )(send)
    return dict(zip(message_order(tokens), outs))


def attention(hist_len, queries, keys, values, tokens, requests):
    slots, width, positions = keys.shape
    heads = queries.shape[0] // tokens
    head_size = width // heads
    blocks = requests // BLOCK_REQUESTS
    lane_tiles = -(-width // 128)
    flops = 4 * requests * LONGEST * heads * heads * tokens * width
    return pl.pallas_call(
        lambda *refs: attention_kernel((tokens, heads, requests, head_size, positions, slots), *refs),
        out_shape=jax.ShapeDtypeStruct((lane_tiles, tokens * heads * requests, 128), jnp.float32),
        in_specs=[pl.BlockSpec(memory_space=pltpu.MemorySpace.HBM)] * 4,
        out_specs=pl.BlockSpec(memory_space=pltpu.VMEM),
        scratch_shapes=[
            pltpu.SMEM(hist_len.shape, jnp.int32),
            pltpu.VMEM(queries.shape, queries.dtype),
            pltpu.VMEM(keys.shape, keys.dtype),
            pltpu.VMEM(values.shape, values.dtype),
            pltpu.VMEM(queries.shape, jnp.float32),
            pltpu.VMEM((heads * heads * tokens, width), jnp.float32),
            pltpu.SMEM((requests,), jnp.int32),
            pltpu.SemaphoreType.DMA((2, blocks)),
            pltpu.SemaphoreType.DMA((2,)),
        ],
        compiler_params=pltpu.CompilerParams(vmem_limit_bytes=16 * MIB),
        cost_estimate=pl.CostEstimate(
            flops=flops, transcendentals=flops // 400, bytes_accessed=2 * keys.size * 2
        ),
        name="attention",
    )(*[pltpu.with_memory_space_constraint(x, pltpu.HBM) for x in (hist_len, queries, keys, values)])


def norm_rows(rows):
    average = jnp.mean(rows, axis=-1, keepdims=True)
    centred = rows - average
    variance = jnp.mean(centred * centred, axis=-1, keepdims=True)
    return centred * lax.rsqrt(variance + EPSILON)


def mix_kernel(sizes, *refs):
    tokens, heads, requests, head_size, j = sizes
    sent = refs[:tokens]
    received = refs[tokens : 2 * tokens]
    gain_ref, out_ref, joined = refs[2 * tokens :]
    mine = lax.axis_index("token")
    for step in range(tokens):
        s = source_of(mine, step, tokens)
        own = sent[peer_step(step, tokens)]
        mixed = jnp.concatenate(
            [
                own[h * requests : (h + 1) * requests, j * head_size : (j + 1) * head_size]
                for h in range(heads)
            ],
            axis=1,
        )
        unmixed = received[step][j * requests : (j + 1) * requests, :]
        joined[s] = mixed.astype(jnp.float32) + unmixed.astype(jnp.float32)
    rows = jnp.concatenate([joined[s] for s in range(tokens)], axis=1)
    out_ref[...] = (norm_rows(rows) * gain_ref[...]).astype(jnp.bfloat16)


def peer_step(step, count):
    if count & (count - 1) == 0:
        return step
    return (count - step) % count


def mix(sent, received, gain, j, tokens, requests):
    heads = sent[0].shape[0] // requests
    width = sent[0].shape[1]
    model = gain.shape[1]
    return pl.pallas_call(
        lambda *refs: mix_kernel((tokens, heads, requests, width // heads, j), *refs),
        out_shape=jax.ShapeDtypeStruct((requests, model), jnp.bfloat16),
        scratch_shapes=[pltpu.VMEM((tokens, requests, width), jnp.float32)],
        compiler_params=pltpu.CompilerParams(vmem_limit_bytes=8 * MIB),
        cost_estimate=pl.CostEstimate(
            flops=10 * requests * model, transcendentals=0, bytes_accessed=6 * requests * model
        ),
        name="mix",
    )(*sent, *received, gain)


def ffn_kernel(sizes, *refs):
    j, peers = sizes
    rows = refs[:peers]
    up_ref, down_ref = refs[peers : peers + 2]
    outs = refs[peers + 2 :]
    x = jnp.concatenate([ref[...] for ref in rows], axis=0)
    lifted = jnp.dot(x, up_ref[j], preferred_element_type=jnp.float32)
    activated = (0.5 * lifted * (1.0 + lax.erf(lifted * math.sqrt(0.5)))).astype(jnp.bfloat16)
    total = jnp.dot(activated, down_ref[j], preferred_element_type=jnp.float32)
    count = rows[0].shape[0]
    for k in range(peers):
        outs[k][...] = total[k * count : (k + 1) * count].astype(outs[k].dtype)


def ffn(rows, w_up, w_down, j):
    _, model, hidden = w_up.shape
    peers = len(rows)
    count = rows[0].shape[0]
    return pl.pallas_call(
        lambda *refs: ffn_kernel((j, peers), *refs),
        out_shape=[
            jax.ShapeDtypeStruct((count, model), jnp.float32 if k == 0 else jnp.bfloat16)
            for k in range(peers)
        ],
        in_specs=[pl.BlockSpec(memory_space=pltpu.VMEM)] * (peers + 2),
        out_specs=[pl.BlockSpec(memory_space=pltpu.VMEM)] * peers,
        compiler_params=pltpu.CompilerParams(vmem_limit_bytes=8 * MIB),
        cost_estimate=pl.CostEstimate(
            flops=4 * peers * count * model * hidden,
            transcendentals=peers * count * hidden,
            bytes_accessed=4 * model * hidden,
        ),
        name="ffn",
    )(*rows, w_up, w_down)


def finish_kernel(sizes, *refs):
    heads, parts = sizes
    gain_ref, out_ref = refs[heads * parts :]
    for j in range(heads):
        summed = refs[j * parts][...]
        for ref in refs[j * parts + 1 : (j + 1) * parts]:
            summed = summed + ref[...].astype(jnp.float32)
        out_ref[:, j, :] = (norm_rows(summed) * gain_ref[...]).astype(jnp.bfloat16)


def finish(terms, gain):
    heads, parts = len(terms), len(terms[0])
    count, model = terms[0][0].shape
    return pl.pallas_call(
        lambda *refs: finish_kernel((heads, parts), *refs),
        out_shape=jax.ShapeDtypeStruct((count, heads, model), jnp.bfloat16),
        compiler_params=pltpu.CompilerParams(vmem_limit_bytes=16 * MIB),
        cost_estimate=pl.CostEstimate(
            flops=10 * heads * count * model, transcendentals=0, bytes_accessed=8 * heads * count * model
        ),
        name="finish",
    )(*[part for token in terms for part in token], gain)


def local(hist_len, queries, history_keys, cached_history_values, gain_mix, w_up, w_down, gain_out):
    tokens = lax.axis_size("token")
    sides = lax.axis_size("hidden")
    groups = lax.axis_size("batch") * sides
    requests = hist_len.shape[0] // groups
    heads = queries.shape[0] // tokens
    w_up = pltpu.with_memory_space_constraint(w_up, pltpu.VMEM)
    w_down = pltpu.with_memory_space_constraint(w_down, pltpu.VMEM)
    send = attention(hist_len, queries, history_keys, cached_history_values, tokens, requests)
    messages = pack(send, tokens, requests, heads, history_keys.shape[1])
    arrived = {0: messages[0]}
    for k in message_order(tokens)[1:]:
        arrived[k] = exchange(messages[k], "token", k, tokens)
    sent = [messages[k] for k in range(tokens)]
    received = [arrived[k] for k in range(tokens)]
    gain_mix = gain_mix.reshape(1, -1)
    gain_out = gain_out.reshape(1, -1)
    normed = [mix(sent, received, gain_mix, j, tokens, requests) for j in range(heads)]
    terms = []
    for j in range(heads):
        rows = [normed[j]] + [exchange(normed[j], "hidden", k, sides) for k in range(1, sides)]
        parts = ffn(rows, w_up, w_down, j)
        back = [
            exchange(parts[k], "hidden", peer_step(k, sides), sides) for k in range(1, sides)
        ]
        terms.append([parts[0]] + back + [normed[j]])
    return finish(terms, gain_out)


def solution(mesh):
    return jax.shard_map(
        local,
        mesh=mesh,
        in_specs=(
            P(),
            P(None, "token"),
            P(("batch", "hidden"), "token", None),
            P(("batch", "hidden"), "token", None),
            P(),
            P("token", None, "hidden"),
            P("token", "hidden", None),
            P(),
        ),
        out_specs=P(("batch", "hidden"), "token", None),
        check_vma=False,
    )
```

```python
import math

import jax
import jax.numpy as jnp
from jax import lax
from jax.experimental import pallas as pl
from jax.experimental.pallas import tpu as pltpu
from jax.sharding import PartitionSpec as P


EPSILON = 1e-05
NEGATIVE_FILL = -1e30
LONGEST = 512
BLOCK_REQUESTS = 4
MIB = 1 << 20


def peer_of(index, step, count):
    if count & (count - 1) == 0:
        return index ^ step
    return (index + step) % count


def source_of(index, step, count):
    if count & (count - 1) == 0:
        return index ^ step
    return (index + count - step) % count


def exchange(value, axis, step, count):
    return lax.ppermute(value, axis, [(a, peer_of(a, step, count)) for a in range(count)])


def attention_kernel(sizes, len_hbm, query_hbm, key_hbm, value_hbm, *rest):
    tokens, heads, requests, head_size, positions, slots = sizes
    send, len_ref, query_ref, key_buf, value_buf, query_f32, query_diag, score_buf, first_ref, sems, small = rest
    width = heads * head_size
    lane_tiles = send.shape[0]
    blocks = requests // BLOCK_REQUESTS
    chunk = slots // blocks
    depth = -(-LONGEST // positions)

    def copies(block):
        where = pl.ds(block * chunk, chunk)
        return (
            pltpu.make_async_copy(key_hbm.at[where], key_buf.at[where], sems.at[0, block]),
            pltpu.make_async_copy(value_hbm.at[where], value_buf.at[where], sems.at[1, block]),
        )

    len_copy = pltpu.make_async_copy(len_hbm, len_ref, small.at[0])
    query_copy = pltpu.make_async_copy(query_hbm, query_ref, small.at[1])
    len_copy.start()
    query_copy.start()
    for block in range(min(3, blocks)):
        for copy in copies(block):
            copy.start()
    len_copy.wait()

    group = lax.axis_index(("batch", "hidden"))
    base = group * requests

    def place(r, first):
        first_ref[r] = first
        return first + (len_ref[base + r] + (positions - 1)) // positions

    lax.fori_loop(0, requests, place, jnp.int32(0))

    query_copy.wait()
    query_f32[...] = query_ref[...].astype(jnp.float32)
    column_head = lax.broadcasted_iota(jnp.int32, (tokens, width), 1) // head_size
    for i in range(heads):
        rows = jnp.concatenate(
            [query_f32[d * heads + i : d * heads + i + 1, :] for d in range(tokens)], axis=0
        )
        for h in range(heads):
            start = (i * heads + h) * tokens
            query_diag[start : start + tokens, :] = jnp.where(column_head == h, rows, 0.0)
    queries = query_diag[...].astype(jnp.bfloat16)
    factor = math.log2(math.e) * head_size ** (-0.5)
    lane = lax.broadcasted_iota(jnp.int32, (1, depth * positions), 1)

    def spans(block):
        last = (block + 1) * chunk - 1
        for offset in range(BLOCK_REQUESTS):
            r = block * BLOCK_REQUESTS + offset
            first = first_ref[r]
            yield offset, r, [jnp.minimum(first + b, last) for b in range(depth)]

    def score(block):
        for offset, r, index in spans(block):
            keys = jnp.concatenate([key_buf[n] for n in index], axis=1)
            score_buf[block % 2, offset] = jnp.dot(
                queries, keys, preferred_element_type=jnp.float32
            )

    def block_body(block, carry):
        following = jnp.minimum(block + 1, blocks - 1)

        @pl.when(block + 1 < blocks)
        def _():
            for copy in copies(block + 1):
                copy.wait()

        @pl.when(block + 3 < blocks)
        def _():
            for copy in copies(block + 3):
                copy.start()

        for offset, r, index in spans(block):
            length = len_ref[base + r]
            values = jnp.concatenate([value_buf[n] for n in index], axis=1)
            scores = jnp.where(lane < length, score_buf[block % 2, offset], NEGATIVE_FILL)
            top = jnp.max(scores, axis=1, keepdims=True)
            terms = jnp.exp2((scores - top) * factor)
            total = jnp.sum(terms, axis=1, keepdims=True)
            acc = lax.dot_general(
                terms.astype(jnp.bfloat16),
                values,
                (((1,), (1,)), ((), ())),
                preferred_element_type=jnp.float32,
            )
            acc = acc / total
            for i in range(heads):
                start = i * heads * tokens
                kept = acc[start : start + tokens]
                for h in range(1, heads):
                    begin = start + h * tokens
                    kept = jnp.where(column_head >= h, acc[begin : begin + tokens], kept)
                spare = lane_tiles * 128 - width
                if spare:
                    kept = jnp.concatenate([kept, jnp.zeros((tokens, spare), jnp.float32)], axis=1)
                for tile in range(lane_tiles):
                    send[tile, pl.ds(i * requests + r, tokens, stride=send.shape[1] // tokens), :] = kept[
                        :, tile * 128 : (tile + 1) * 128
                    ]
        score(following)
        return carry

    for copy in copies(0):
        copy.wait()
    score(0)
    lax.fori_loop(0, blocks, block_body, jnp.int32(0))


def pack_kernel(sizes, send, *outs):
    tokens, rows, width = sizes
    lane_tiles = send.shape[0]
    pitch = send.shape[1] // tokens
    mine = lax.axis_index("token")
    for out, step in zip(outs, message_order(tokens)):
        d = peer_of(mine, step, tokens)
        where = pl.ds(pl.multiple_of(d * pitch, 8), rows)
        values = jnp.concatenate([send[tile, where, :] for tile in range(lane_tiles)], axis=1)
        out[...] = values[:, :width].astype(jnp.bfloat16)


def message_order(tokens):
    return [0] + list(range(tokens - 1, 0, -1))


def pack(send, tokens, requests, heads, width):
    rows = heads * requests
    outs = pl.pallas_call(
        lambda *refs: pack_kernel((tokens, rows, width), *refs),
        out_shape=[jax.ShapeDtypeStruct((rows, width), jnp.bfloat16)] * tokens,
        in_specs=[pl.BlockSpec(memory_space=pltpu.VMEM)],
        out_specs=[pl.BlockSpec(memory_space=pltpu.VMEM)] * tokens,
        compiler_params=pltpu.CompilerParams(vmem_limit_bytes=4 * MIB),
        cost_estimate=pl.CostEstimate(
            flops=30_000_000_000, transcendentals=0, bytes_accessed=200_000_000
        ),
        name="pack",
    )(send)
    return dict(zip(message_order(tokens), outs))


def attention(hist_len, queries, keys, values, tokens, requests):
    slots, width, positions = keys.shape
    heads = queries.shape[0] // tokens
    head_size = width // heads
    blocks = requests // BLOCK_REQUESTS
    lane_tiles = -(-width // 128)
    flops = 4 * requests * LONGEST * heads * heads * tokens * width
    return pl.pallas_call(
        lambda *refs: attention_kernel((tokens, heads, requests, head_size, positions, slots), *refs),
        out_shape=jax.ShapeDtypeStruct(
            (lane_tiles, tokens * (heads * requests + 8), 128), jnp.float32
        ),
        in_specs=[pl.BlockSpec(memory_space=pltpu.MemorySpace.HBM)] * 4,
        out_specs=pl.BlockSpec(memory_space=pltpu.VMEM),
        scratch_shapes=[
            pltpu.SMEM(hist_len.shape, jnp.int32),
            pltpu.VMEM(queries.shape, queries.dtype),
            pltpu.VMEM(keys.shape, keys.dtype),
            pltpu.VMEM(values.shape, values.dtype),
            pltpu.VMEM(queries.shape, jnp.float32),
            pltpu.VMEM((heads * heads * tokens, width), jnp.float32),
            pltpu.VMEM(
                (2, BLOCK_REQUESTS, heads * heads * tokens, -(-LONGEST // positions) * positions),
                jnp.float32,
            ),
            pltpu.SMEM((requests,), jnp.int32),
            pltpu.SemaphoreType.DMA((2, blocks)),
            pltpu.SemaphoreType.DMA((2,)),
        ],
        compiler_params=pltpu.CompilerParams(vmem_limit_bytes=16 * MIB),
        cost_estimate=pl.CostEstimate(
            flops=flops, transcendentals=flops // 400, bytes_accessed=2 * keys.size * 2
        ),
        name="attention",
    )(*[pltpu.with_memory_space_constraint(x, pltpu.HBM) for x in (hist_len, queries, keys, values)])


def norm_rows(rows):
    average = jnp.mean(rows, axis=-1, keepdims=True)
    centred = rows - average
    variance = jnp.mean(centred * centred, axis=-1, keepdims=True)
    return centred * lax.rsqrt(variance + EPSILON)


def mix_kernel(sizes, *refs):
    tokens, heads, requests, head_size, j = sizes
    sent = refs[:tokens]
    received = refs[tokens : 2 * tokens]
    gain_ref, out_ref, joined = refs[2 * tokens :]
    mine = lax.axis_index("token")
    for step in range(tokens):
        s = source_of(mine, step, tokens)
        own = sent[peer_step(step, tokens)]
        mixed = jnp.concatenate(
            [
                own[h * requests : (h + 1) * requests, j * head_size : (j + 1) * head_size]
                for h in range(heads)
            ],
            axis=1,
        )
        unmixed = received[step][j * requests : (j + 1) * requests, :]
        joined[s] = mixed.astype(jnp.float32) + unmixed.astype(jnp.float32)
    rows = jnp.concatenate([joined[s] for s in range(tokens)], axis=1)
    out_ref[...] = (norm_rows(rows) * gain_ref[...]).astype(jnp.bfloat16)


def peer_step(step, count):
    if count & (count - 1) == 0:
        return step
    return (count - step) % count


def mix(sent, received, gain, j, tokens, requests):
    heads = sent[0].shape[0] // requests
    width = sent[0].shape[1]
    model = gain.shape[1]
    return pl.pallas_call(
        lambda *refs: mix_kernel((tokens, heads, requests, width // heads, j), *refs),
        out_shape=jax.ShapeDtypeStruct((requests, model), jnp.bfloat16),
        scratch_shapes=[pltpu.VMEM((tokens, requests, width), jnp.float32)],
        compiler_params=pltpu.CompilerParams(vmem_limit_bytes=8 * MIB),
        cost_estimate=pl.CostEstimate(
            flops=10 * requests * model, transcendentals=0, bytes_accessed=6 * requests * model
        ),
        name="mix",
    )(*sent, *received, gain)


def ffn_kernel(sizes, *refs):
    j, peers = sizes
    rows = refs[:peers]
    up_ref, down_ref = refs[peers : peers + 2]
    outs = refs[peers + 2 :]
    x = jnp.concatenate([ref[...] for ref in rows], axis=0)
    lifted = jnp.dot(x, up_ref[j], preferred_element_type=jnp.float32)
    activated = (0.5 * lifted * (1.0 + lax.erf(lifted * math.sqrt(0.5)))).astype(jnp.bfloat16)
    total = jnp.dot(activated, down_ref[j], preferred_element_type=jnp.float32)
    count = rows[0].shape[0]
    for k in range(peers):
        outs[k][...] = total[k * count : (k + 1) * count].astype(outs[k].dtype)


def ffn(rows, w_up, w_down, j):
    _, model, hidden = w_up.shape
    peers = len(rows)
    count = rows[0].shape[0]
    return pl.pallas_call(
        lambda *refs: ffn_kernel((j, peers), *refs),
        out_shape=[
            jax.ShapeDtypeStruct((count, model), jnp.float32 if k == 0 else jnp.bfloat16)
            for k in range(peers)
        ],
        in_specs=[pl.BlockSpec(memory_space=pltpu.VMEM)] * (peers + 2),
        out_specs=[pl.BlockSpec(memory_space=pltpu.VMEM)] * peers,
        compiler_params=pltpu.CompilerParams(vmem_limit_bytes=8 * MIB),
        cost_estimate=pl.CostEstimate(
            flops=4 * peers * count * model * hidden,
            transcendentals=peers * count * hidden,
            bytes_accessed=4 * model * hidden,
        ),
        name="ffn",
    )(*rows, w_up, w_down)


def finish_kernel(sizes, *refs):
    heads, parts = sizes
    gain_ref, out_ref = refs[heads * parts :]
    for j in range(heads):
        summed = refs[j * parts][...]
        for ref in refs[j * parts + 1 : (j + 1) * parts]:
            summed = summed + ref[...].astype(jnp.float32)
        out_ref[:, j, :] = (norm_rows(summed) * gain_ref[...]).astype(jnp.bfloat16)


def finish(terms, gain):
    heads, parts = len(terms), len(terms[0])
    count, model = terms[0][0].shape
    return pl.pallas_call(
        lambda *refs: finish_kernel((heads, parts), *refs),
        out_shape=jax.ShapeDtypeStruct((count, heads, model), jnp.bfloat16),
        compiler_params=pltpu.CompilerParams(vmem_limit_bytes=16 * MIB),
        cost_estimate=pl.CostEstimate(
            flops=10 * heads * count * model, transcendentals=0, bytes_accessed=8 * heads * count * model
        ),
        name="finish",
    )(*[part for token in terms for part in token], gain)


def local(hist_len, queries, history_keys, cached_history_values, gain_mix, w_up, w_down, gain_out):
    tokens = lax.axis_size("token")
    sides = lax.axis_size("hidden")
    groups = lax.axis_size("batch") * sides
    requests = hist_len.shape[0] // groups
    heads = queries.shape[0] // tokens
    w_up = pltpu.with_memory_space_constraint(w_up, pltpu.VMEM)
    w_down = pltpu.with_memory_space_constraint(w_down, pltpu.VMEM)
    send = attention(hist_len, queries, history_keys, cached_history_values, tokens, requests)
    messages = pack(send, tokens, requests, heads, history_keys.shape[1])
    arrived = {0: messages[0]}
    for k in message_order(tokens)[1:]:
        arrived[k] = exchange(messages[k], "token", k, tokens)
    sent = [messages[k] for k in range(tokens)]
    received = [arrived[k] for k in range(tokens)]
    gain_mix = gain_mix.reshape(1, -1)
    gain_out = gain_out.reshape(1, -1)
    normed = [mix(sent, received, gain_mix, j, tokens, requests) for j in range(heads)]
    terms = []
    for j in range(heads):
        rows = [normed[j]] + [exchange(normed[j], "hidden", k, sides) for k in range(1, sides)]
        parts = ffn(rows, w_up, w_down, j)
        back = [
            exchange(parts[k], "hidden", peer_step(k, sides), sides) for k in range(1, sides)
        ]
        terms.append([parts[0]] + back + [normed[j]])
    return finish(terms, gain_out)


def solution(mesh):
    return jax.shard_map(
        local,
        mesh=mesh,
        in_specs=(
            P(),
            P(None, "token"),
            P(("batch", "hidden"), "token", None),
            P(("batch", "hidden"), "token", None),
            P(),
            P("token", None, "hidden"),
            P("token", "hidden", None),
            P(),
        ),
        out_specs=P(("batch", "hidden"), "token", None),
        check_vma=False,
    )
```

```python
import math

import jax
import jax.numpy as jnp
from jax import lax
from jax.experimental import pallas as pl
from jax.experimental.pallas import tpu as pltpu
from jax.sharding import PartitionSpec as P


EPSILON = 1e-05
NEGATIVE_FILL = -1e30
LONGEST = 512
BLOCK_REQUESTS = 4
MIB = 1 << 20


def peer_of(index, step, count):
    if count & (count - 1) == 0:
        return index ^ step
    return (index + step) % count


def source_of(index, step, count):
    if count & (count - 1) == 0:
        return index ^ step
    return (index + count - step) % count


def exchange(value, axis, step, count):
    return lax.ppermute(value, axis, [(a, peer_of(a, step, count)) for a in range(count)])


def attention_kernel(sizes, len_hbm, query_hbm, key_hbm, value_hbm, *rest):
    tokens, heads, requests, head_size, positions, slots = sizes
    send, len_ref, query_ref, key_buf, value_buf, query_f32, query_diag, score_buf, first_ref, sems, small = rest
    width = heads * head_size
    lane_tiles = send.shape[0]
    blocks = requests // BLOCK_REQUESTS
    chunk = slots // blocks
    depth = -(-LONGEST // positions)

    def copies(block):
        where = pl.ds(block * chunk, chunk)
        return (
            pltpu.make_async_copy(key_hbm.at[where], key_buf.at[where], sems.at[0, block]),
            pltpu.make_async_copy(value_hbm.at[where], value_buf.at[where], sems.at[1, block]),
        )

    len_copy = pltpu.make_async_copy(len_hbm, len_ref, small.at[0])
    query_copy = pltpu.make_async_copy(query_hbm, query_ref, small.at[1])
    len_copy.start()
    query_copy.start()
    for block in range(min(3, blocks)):
        for copy in copies(block):
            copy.start()
    len_copy.wait()

    group = lax.axis_index(("batch", "hidden"))
    base = group * requests

    def place(r, first):
        first_ref[r] = first
        return first + (len_ref[base + r] + (positions - 1)) // positions

    lax.fori_loop(0, requests, place, jnp.int32(0))

    query_copy.wait()
    query_f32[...] = query_ref[...].astype(jnp.float32)
    column_head = lax.broadcasted_iota(jnp.int32, (tokens, width), 1) // head_size
    for i in range(heads):
        rows = jnp.concatenate(
            [query_f32[d * heads + i : d * heads + i + 1, :] for d in range(tokens)], axis=0
        )
        for h in range(heads):
            start = (i * heads + h) * tokens
            query_diag[start : start + tokens, :] = jnp.where(column_head == h, rows, 0.0)
    queries = query_diag[...].astype(jnp.bfloat16)
    factor = math.log2(math.e) * head_size ** (-0.5)
    lane = lax.broadcasted_iota(jnp.int32, (1, depth * positions), 1)

    def spans(block):
        last = (block + 1) * chunk - 1
        for offset in range(BLOCK_REQUESTS):
            r = block * BLOCK_REQUESTS + offset
            first = first_ref[r]
            yield offset, r, [jnp.minimum(first + b, last) for b in range(depth)]

    def score(block):
        for offset, r, index in spans(block):
            keys = jnp.concatenate([key_buf[n] for n in index], axis=1)
            score_buf[block % 2, offset] = jnp.dot(
                queries, keys, preferred_element_type=jnp.float32
            )

    def block_body(block, carry):
        following = jnp.minimum(block + 1, blocks - 1)

        @pl.when(block + 1 < blocks)
        def _():
            for copy in copies(block + 1):
                copy.wait()

        @pl.when(block + 3 < blocks)
        def _():
            for copy in copies(block + 3):
                copy.start()

        for offset, r, index in spans(block):
            length = len_ref[base + r]
            values = jnp.concatenate([value_buf[n] for n in index], axis=1)
            scores = jnp.where(lane < length, score_buf[block % 2, offset], NEGATIVE_FILL)
            top = jnp.max(scores, axis=1, keepdims=True)
            terms = jnp.exp2((scores - top) * factor)
            total = jnp.sum(terms, axis=1, keepdims=True)
            acc = lax.dot_general(
                terms.astype(jnp.bfloat16),
                values,
                (((1,), (1,)), ((), ())),
                preferred_element_type=jnp.float32,
            )
            acc = acc / total
            for i in range(heads):
                start = i * heads * tokens
                kept = acc[start : start + tokens]
                for h in range(1, heads):
                    begin = start + h * tokens
                    kept = jnp.where(column_head >= h, acc[begin : begin + tokens], kept)
                spare = lane_tiles * 128 - width
                if spare:
                    kept = jnp.concatenate([kept, jnp.zeros((tokens, spare), jnp.float32)], axis=1)
                for tile in range(lane_tiles):
                    send[tile, pl.ds(i * requests + r, tokens, stride=send.shape[1] // tokens), :] = kept[
                        :, tile * 128 : (tile + 1) * 128
                    ]
        score(following)
        return carry

    for copy in copies(0):
        copy.wait()
    score(0)
    lax.fori_loop(0, blocks, block_body, jnp.int32(0))


def pack_kernel(sizes, send, *outs):
    tokens, rows, width = sizes
    lane_tiles = send.shape[0]
    pitch = send.shape[1] // tokens
    mine = lax.axis_index("token")
    for out, step in zip(outs, message_order(tokens)):
        d = peer_of(mine, step, tokens)
        where = pl.ds(pl.multiple_of(d * pitch, 8), rows)
        values = jnp.concatenate([send[tile, where, :] for tile in range(lane_tiles)], axis=1)
        out[...] = values[:, :width].astype(jnp.bfloat16)


def message_order(tokens):
    return [0] + list(range(tokens - 1, 0, -1))


def pack(send, tokens, requests, heads, width):
    rows = heads * requests
    outs = pl.pallas_call(
        lambda *refs: pack_kernel((tokens, rows, width), *refs),
        out_shape=[jax.ShapeDtypeStruct((rows, width), jnp.bfloat16)] * tokens,
        in_specs=[pl.BlockSpec(memory_space=pltpu.VMEM)],
        out_specs=[pl.BlockSpec(memory_space=pltpu.VMEM)] * tokens,
        compiler_params=pltpu.CompilerParams(vmem_limit_bytes=4 * MIB),
        cost_estimate=pl.CostEstimate(
            flops=30_000_000_000, transcendentals=0, bytes_accessed=200_000_000
        ),
        name="pack",
    )(send)
    return dict(zip(message_order(tokens), outs))


def attention(hist_len, queries, keys, values, tokens, requests):
    slots, width, positions = keys.shape
    heads = queries.shape[0] // tokens
    head_size = width // heads
    blocks = requests // BLOCK_REQUESTS
    lane_tiles = -(-width // 128)
    flops = 4 * requests * LONGEST * heads * heads * tokens * width
    return pl.pallas_call(
        lambda *refs: attention_kernel((tokens, heads, requests, head_size, positions, slots), *refs),
        out_shape=jax.ShapeDtypeStruct(
            (lane_tiles, tokens * (heads * requests + 8), 128), jnp.float32
        ),
        in_specs=[pl.BlockSpec(memory_space=pltpu.MemorySpace.HBM)] * 4,
        out_specs=pl.BlockSpec(memory_space=pltpu.VMEM),
        scratch_shapes=[
            pltpu.SMEM(hist_len.shape, jnp.int32),
            pltpu.VMEM(queries.shape, queries.dtype),
            pltpu.VMEM(keys.shape, keys.dtype),
            pltpu.VMEM(values.shape, values.dtype),
            pltpu.VMEM(queries.shape, jnp.float32),
            pltpu.VMEM((heads * heads * tokens, width), jnp.float32),
            pltpu.VMEM(
                (2, BLOCK_REQUESTS, heads * heads * tokens, -(-LONGEST // positions) * positions),
                jnp.float32,
            ),
            pltpu.SMEM((requests,), jnp.int32),
            pltpu.SemaphoreType.DMA((2, blocks)),
            pltpu.SemaphoreType.DMA((2,)),
        ],
        compiler_params=pltpu.CompilerParams(vmem_limit_bytes=16 * MIB),
        cost_estimate=pl.CostEstimate(
            flops=flops, transcendentals=flops // 400, bytes_accessed=2 * keys.size * 2
        ),
        name="attention",
    )(*[pltpu.with_memory_space_constraint(x, pltpu.HBM) for x in (hist_len, queries, keys, values)])


def norm_rows(rows):
    average = jnp.mean(rows, axis=-1, keepdims=True)
    centred = rows - average
    variance = jnp.mean(centred * centred, axis=-1, keepdims=True)
    return centred * lax.rsqrt(variance + EPSILON)


def mix_kernel(sizes, *refs):
    tokens, heads, requests, head_size, j = sizes
    sent = refs[:tokens]
    received = refs[tokens : 2 * tokens]
    gain_ref, out_ref, joined = refs[2 * tokens :]
    mine = lax.axis_index("token")
    for step in range(tokens):
        s = source_of(mine, step, tokens)
        own = sent[peer_step(step, tokens)]
        mixed = jnp.concatenate(
            [
                own[h * requests : (h + 1) * requests, j * head_size : (j + 1) * head_size]
                for h in range(heads)
            ],
            axis=1,
        )
        unmixed = received[step][j * requests : (j + 1) * requests, :]
        joined[s] = mixed.astype(jnp.float32) + unmixed.astype(jnp.float32)
    rows = jnp.concatenate([joined[s] for s in range(tokens)], axis=1)
    out_ref[...] = (norm_rows(rows) * gain_ref[...]).astype(jnp.bfloat16)


def peer_step(step, count):
    if count & (count - 1) == 0:
        return step
    return (count - step) % count


def mix(sent, received, gain, j, tokens, requests):
    heads = sent[0].shape[0] // requests
    width = sent[0].shape[1]
    model = gain.shape[1]
    return pl.pallas_call(
        lambda *refs: mix_kernel((tokens, heads, requests, width // heads, j), *refs),
        out_shape=jax.ShapeDtypeStruct((requests, model), jnp.bfloat16),
        scratch_shapes=[pltpu.VMEM((tokens, requests, width), jnp.float32)],
        compiler_params=pltpu.CompilerParams(vmem_limit_bytes=8 * MIB),
        cost_estimate=pl.CostEstimate(
            flops=10 * requests * model, transcendentals=0, bytes_accessed=6 * requests * model
        ),
        name="mix",
    )(*sent, *received, gain)


def ffn_kernel(sizes, *refs):
    j, peers, place = sizes
    rows = refs[:peers]
    up_ref, down_ref = refs[peers : peers + 2]
    outs = refs[-peers:]
    x = jnp.concatenate([ref[...] for ref in rows], axis=0)
    lifted = jnp.dot(x, up_ref[j], preferred_element_type=jnp.float32)
    activated = (0.5 * lifted * (1.0 + lax.erf(lifted * math.sqrt(0.5)))).astype(jnp.bfloat16)
    total = jnp.dot(activated, down_ref[j], preferred_element_type=jnp.float32)
    count = rows[0].shape[0]
    outs[0][...] = total[:count]
    for k in range(1, peers):
        outs[k][place * count : (place + 1) * count, :] = total[k * count : (k + 1) * count].astype(
            outs[k].dtype
        )


def ffn(rows, w_up, w_down, j, place, together, carried):
    _, model, hidden = w_up.shape
    peers = len(rows)
    count = rows[0].shape[0]
    return pl.pallas_call(
        lambda *refs: ffn_kernel((j, peers, place), *refs),
        out_shape=[jax.ShapeDtypeStruct((count, model), jnp.float32)]
        + [jax.ShapeDtypeStruct((together * count, model), jnp.bfloat16)] * (peers - 1),
        in_specs=[pl.BlockSpec(memory_space=pltpu.VMEM)] * (peers + 2 + len(carried)),
        out_specs=[pl.BlockSpec(memory_space=pltpu.VMEM)] * peers,
        input_output_aliases={peers + 2 + n: 1 + n for n in range(len(carried))},
        compiler_params=pltpu.CompilerParams(vmem_limit_bytes=8 * MIB),
        cost_estimate=pl.CostEstimate(
            flops=4 * peers * count * model * hidden,
            transcendentals=peers * count * hidden,
            bytes_accessed=4 * model * hidden,
        ),
        name="ffn",
    )(*rows, w_up, w_down, *carried)


def finished(own, normed, back, place, gain_ref):
    count = own.shape[0]
    summed = own[...] + normed[...].astype(jnp.float32)
    for ref in back:
        summed = summed + ref[place * count : (place + 1) * count, :].astype(jnp.float32)
    return norm_rows(summed) * gain_ref[...]


def finish_kernel(sizes, last, *refs):
    together, done = sizes
    own, normed = refs[:together], refs[together : 2 * together]
    back = refs[2 * together : len(refs) - (1 if last else together) - 1 - done]
    early = refs[2 * together + len(back) : 2 * together + len(back) + done]
    gain_ref = refs[2 * together + len(back) + done]
    outs = refs[2 * together + len(back) + done + 1 :]
    if last:
        for j, ref in enumerate(early):
            outs[0][:, j, :] = ref[...].astype(jnp.bfloat16)
    for place in range(together):
        rows = finished(own[place], normed[place], back, place, gain_ref)
        if last:
            outs[0][:, done + place, :] = rows.astype(jnp.bfloat16)
        else:
            outs[place][...] = rows


def finish(groups, gain):
    done = []
    for n, (own, normed, back) in enumerate(groups):
        last = n == len(groups) - 1
        together = len(own)
        count, model = own[0].shape
        early = done if last else []
        if last:
            shape = jax.ShapeDtypeStruct((count, len(done) + together, model), jnp.bfloat16)
        else:
            shape = [jax.ShapeDtypeStruct((count, model), jnp.float32)] * together
        args = [*own, *normed, *back, *early, gain]
        sizes = (together, len(early))
        out = pl.pallas_call(
            lambda *refs, sizes=sizes, last=last: finish_kernel(sizes, last, *refs),
            out_shape=shape,
            compiler_params=pltpu.CompilerParams(vmem_limit_bytes=16 * MIB),
            cost_estimate=pl.CostEstimate(
                flops=10 * together * count * model,
                transcendentals=0,
                bytes_accessed=8 * together * count * model,
            ),
            name="finish" if last else "finish_early",
        )(*args)
        if not last:
            done.extend(out)
    return out


def local(hist_len, queries, history_keys, cached_history_values, gain_mix, w_up, w_down, gain_out):
    tokens = lax.axis_size("token")
    sides = lax.axis_size("hidden")
    groups = lax.axis_size("batch") * sides
    requests = hist_len.shape[0] // groups
    heads = queries.shape[0] // tokens
    w_up = pltpu.with_memory_space_constraint(w_up, pltpu.VMEM)
    w_down = pltpu.with_memory_space_constraint(w_down, pltpu.VMEM)
    send = attention(hist_len, queries, history_keys, cached_history_values, tokens, requests)
    messages = pack(send, tokens, requests, heads, history_keys.shape[1])
    arrived = {0: messages[0]}
    for k in message_order(tokens)[1:]:
        arrived[k] = exchange(messages[k], "token", k, tokens)
    sent = [messages[k] for k in range(tokens)]
    received = [arrived[k] for k in range(tokens)]
    gain_mix = gain_mix.reshape(1, -1)
    gain_out = gain_out.reshape(1, -1)
    normed = [mix(sent, received, gain_mix, j, tokens, requests) for j in range(heads)]
    together = 2 if heads % 2 == 0 else 1
    groups = []
    for start in range(0, heads, together):
        own, carried = [], []
        for place in range(together):
            j = start + place
            rows = [normed[j]] + [exchange(normed[j], "hidden", k, sides) for k in range(1, sides)]
            part, *carried = ffn(rows, w_up, w_down, j, place, together, carried)
            own.append(part)
        back = [
            exchange(carried[k - 1], "hidden", peer_step(k, sides), sides) for k in range(1, sides)
        ]
        groups.append((own, normed[start : start + together], back))
    return finish(groups, gain_out)


def solution(mesh):
    return jax.shard_map(
        local,
        mesh=mesh,
        in_specs=(
            P(),
            P(None, "token"),
            P(("batch", "hidden"), "token", None),
            P(("batch", "hidden"), "token", None),
            P(),
            P("token", None, "hidden"),
            P("token", "hidden", None),
            P(),
        ),
        out_specs=P(("batch", "hidden"), "token", None),
        check_vma=False,
    )
```
